32 devices in a mesh: dp: 2 (over x), expert: 4 (over y, core), sample: 4 (over z).
Axes of the slice: x: 2, y: 2, z: 4, core: 2. Of those that a mesh axis runs over, the one named last changes fastest.
Arguments:
- tokens: bfloat16 [640, 4096], P(('dp', 'expert', 'sample')), may hold values from -6 to 6
- cotangent: bfloat16 [640, 4096], P(('dp', 'expert', 'sample')), may hold values from -6 to 6
- routes: int32 [640, 2], P(('dp', 'expert', 'sample')), may hold values from 0 to 7, all different within a row; in each aligned block of 20 rows (0 to 19, 20 to 39, ...) at most 6 rows name the same one
- gate_weights: float32 [640, 2], P(('dp', 'expert', 'sample')), may hold values from 0.1 to 1
- lengths: int32 [8, 4], P(('dp', 'expert'), 'sample'), may hold values from 1 to 20
- rewards: int32 [8, 4], P(('dp', 'expert'), 'sample'), may hold values from -48 to 48
- w_gate: bfloat16 [8, 8192, 4096], P('expert', ('dp', 'sample')), may hold values from -0.09375 to 0.09375
- w_up: bfloat16 [8, 8192, 4096], P('expert', ('dp', 'sample')), may hold values from -0.09375 to 0.09375
- w_down: bfloat16 [8, 8192, 4096], P('expert', ('dp', 'sample')), may hold values from -0.0625 to 0.0625
Outputs:
- grad_tokens: bfloat16 [640, 4096], P(('dp', 'expert', 'sample'))
- grad_w_gate: bfloat16 [8, 8192, 4096], P('expert', ('dp', 'sample'))
- grad_w_up: bfloat16 [8, 8192, 4096], P('expert', ('dp', 'sample'))
- grad_w_down: bfloat16 [8, 8192, 4096], P('expert', ('dp', 'sample'))
The draws below stay inside these ranges and needn't reach their ends.
Inputs may be any that keep to these rules, and one draw needn't show every extreme that they name: `routes`: each row names 2 different experts; among the rows of one device no expert is named by more than 6 rows, and in every draw some device's rows name some expert exactly 6 times.
All inputs are finite; a program needn't handle non-finite values.
Results may differ from the reference program's by a relative error of at most 0.025.
Values may be sent and summed in bfloat16 or wider, within the bound.
A program may use at most 192 MiB of HBM per device.

```python
import math
import jax
import jax.numpy as jnp
import numpy as np
from jax import lax

D = 4096
FF = 8192
EXPERTS = 8
TOP = 2
TOK_DEV = 20
CAP = 6
K = 4
PROMPTS = 8
TOKENS = 640
N_DP = 2
N_EXPERT = 4
N_SAMPLE = 4


def touch_ends(drawn, rng, low, top_value):
    longest = drawn.shape.index(max(drawn.shape))
    spots = []
    for shift in (0, 1):
        where = [jax.random.randint(jax.random.fold_in(rng, axis), (), 0, length) for axis, length in enumerate(drawn.shape)]
        where[longest] = (where[longest] + shift) % drawn.shape[longest]
        spots.append(tuple(where))
    return drawn.at[spots[0]].set(low).at[spots[1]].set(top_value)


def block_scale(rng, shape, pieces, smallest, top_value):
    def one(dim, parts):
        heights = jax.random.uniform(jax.random.fold_in(jax.random.fold_in(rng, 6), dim), (parts,), jnp.float32, smallest / len(pieces), top_value / len(pieces))
        return jnp.repeat(jnp.exp(heights), shape[dim] // parts).reshape((-1,) + (1,) * (len(shape) - dim - 1))

    loudness = one(*pieces[0])
    for cut in pieces[1:]:
        loudness = loudness * one(*cut)
    return loudness


def shared_out(rng, own, number, rows, count, top, most, skew):
    ranking = jax.random.permutation(rng, count)
    crowded, usual = portions_of(count, rows * top, most, skew, True), portions_of(count, rows * top, most, skew, False)
    places = jnp.arange(count)

    def named(sizes, offset_by):
        used = int((sizes > 0).sum())
        fixed = max(1, used // 4)
        passed = fixed + (places - fixed + offset_by * (used - fixed)) % max(1, count - fixed)
        return jnp.zeros((count,), jnp.int32).at[ranking[jnp.where(places < fixed, places, passed)]].set(jnp.asarray(sizes, jnp.int32))

    sizes = jnp.where(number % 4 == 0, named(crowded, number // 4), named(usual, number - number // 4 - 1))
    mixed = jax.random.permutation(jax.random.fold_in(own, 3), count)
    giver, receiver = mixed[0:count // 2 * 2:2], mixed[1:count // 2 * 2:2]
    margin = jnp.minimum(sizes[giver] - 1, most - sizes[receiver]) // 2
    margin = jnp.where((giver == ranking[0]) | (receiver == ranking[0]) | (sizes[receiver] == 0), 0, jnp.maximum(margin, 0))
    passed = jax.random.randint(jax.random.fold_in(own, 4), (count // 2,), 0, 1 << 20) % (margin + 1)
    sizes = sizes.at[giver].add(-passed).at[receiver].add(passed)
    labels = jnp.searchsorted(jnp.cumsum(sizes), jnp.arange(rows * top), side="right").astype(jnp.int32)
    grid = labels.reshape(top, rows).T
    grid = grid[jax.random.permutation(jax.random.fold_in(own, 1), rows)]
    offset_by = jax.random.randint(jax.random.fold_in(own, 2), (rows, 1), 0, top)
    return jnp.take_along_axis(grid, (jnp.arange(top)[None, :] + offset_by) % top, axis=1)


def portions_of(amount, total, bound, skew, full):
    weights = [(1 << 20) // math.isqrt(standing ** skew) + 1 for standing in range(1, amount + 1)]
    largest = bound if full else min(bound, max(-(-total // amount), total * weights[0] // sum(weights)))
    least = 1 if total - largest >= amount - 1 else 0
    holding, spare = [largest] + [least] * (amount - 1), total - largest - least * (amount - 1)
    while spare > 0:
        candidates = [i for i in range(1, amount) if holding[i] < largest] or [i for i in range(1, amount) if holding[i] < bound]
        whole, budget = sum([weights[i] for i in candidates]), spare
        for i in candidates:
            more = min(bound - holding[i], max(1, budget * weights[i] // whole), spare)
            holding[i] = holding[i] + more
            spare = spare - more
    return np.array(holding)


def centred(key, dims, spread, reach, shards=(), kind=jnp.bfloat16):
    gain = block_scale(key, dims, shards, -0.22, 0.18) if shards else 1.0
    array = jax.random.normal(key, dims, jnp.float32) * spread * gain
    return jnp.minimum(jnp.maximum(array, -reach), reach).astype(kind)


def setup_inputs(seed: int = 0) -> dict:
    streams_of = jax.random.split(jax.random.key(seed), 10)
    tokens = centred(streams_of[0], (TOKENS, D), 1.0, 6.0, ((0, 32),))
    cotangent = centred(streams_of[1], (TOKENS, D), 1.0, 6.0, ((0, 32),))
    routes_keys = jax.random.split(jax.random.fold_in(streams_of[2], 1), TOKENS // TOK_DEV)
    routes_turns = jax.random.permutation(jax.random.fold_in(streams_of[2], 3), TOKENS // TOK_DEV)
    routes = jax.vmap(lambda own, number: shared_out(jax.random.fold_in(streams_of[2], 2), own, number, TOK_DEV, EXPERTS, TOP, CAP, 2))(routes_keys, routes_turns).reshape((TOKENS, TOP))
    gate_weights = jnp.clip(0.1 + 0.9 * jax.random.uniform(streams_of[3], (TOKENS, TOP), jnp.float32) ** block_scale(streams_of[3], (TOKENS, TOP), ((0, 32),), -0.2, 0.2), 0.1, 1.0)
    lengths = touch_ends(jax.random.randint(streams_of[4], (PROMPTS, K), 1, TOK_DEV + 1), jax.random.fold_in(streams_of[4], 1), 1, TOK_DEV).astype(jnp.int32)
    rewards = touch_ends(jax.random.randint(streams_of[5], (PROMPTS, K), -48, 49), jax.random.fold_in(streams_of[5], 1), -48, 48).astype(jnp.int32)
    w_gate = centred(streams_of[6], (EXPERTS, FF, D), D ** -0.5, 0.09375, ((0, 4), (1, 8)))
    w_up = centred(streams_of[7], (EXPERTS, FF, D), D ** -0.5, 0.09375, ((0, 4), (1, 8)))
    w_down = centred(streams_of[8], (EXPERTS, FF, D), FF ** -0.5, 0.0625, ((0, 4), (1, 8)))
    return dict(tokens=tokens, cotangent=cotangent, routes=routes, gate_weights=gate_weights, lengths=lengths, rewards=rewards, w_gate=w_gate, w_up=w_up, w_down=w_down)


def silu_parts(pre_gate):
    gate_prob = jax.nn.sigmoid(pre_gate)
    return pre_gate * gate_prob, gate_prob * (1.0 + pre_gate * (1.0 - gate_prob))


def reference(tokens, cotangent, routes, gate_weights, lengths, rewards, w_gate, w_up, w_down):
    devices = N_DP * N_EXPERT * N_SAMPLE
    slices = N_DP * N_SAMPLE
    width_slice = FF // slices
    choices_per = routes.shape[1]
    reward = rewards.astype(jnp.float32) * 0.0625
    reward_total = jnp.sum(reward, axis=1, keepdims=True)
    advantage = reward - (reward_total - reward) / (K - 1)
    owner = jnp.arange(TOKENS, dtype=jnp.int32) // TOK_DEV
    position = jnp.arange(TOKENS, dtype=jnp.int32) % TOK_DEV
    live = position < lengths.reshape(-1)[owner]
    weight_row = jnp.where(live, -advantage.reshape(-1)[owner], jnp.zeros((), jnp.float32))
    pair_scale = (gate_weights * weight_row[:, None]).reshape(-1)
    pair_expert = routes.reshape(-1)
    pair_count = pair_expert.shape[0]
    limit = devices * CAP
    member = (pair_expert[:, None] == jnp.arange(EXPERTS, dtype=jnp.int32)[None, :]).astype(jnp.int32)
    order = jnp.cumsum(member, axis=0) - 1
    where_row = jnp.where(member > 0, order, limit).astype(jnp.int32)
    pair_ids = jnp.broadcast_to(jnp.arange(pair_count, dtype=jnp.int32)[:, None], member.shape)
    expert_ids = jnp.broadcast_to(jnp.arange(EXPERTS, dtype=jnp.int32)[None, :], member.shape)
    table = jnp.zeros((EXPERTS, limit), jnp.int32).at[expert_ids, where_row].set(pair_ids, mode="drop")
    filled = jnp.arange(limit, dtype=jnp.int32)[None, :] < jnp.sum(member, axis=0)[:, None]

    def one_expert(packed):
        pair_rows, valid, gate_rows, up_rows, down_rows = packed
        token_rows = pair_rows // choices_per
        inputs = tokens[token_rows]
        scale = jnp.where(valid, pair_scale[pair_rows], jnp.zeros((), jnp.float32))
        grads_out = (cotangent[token_rows].astype(jnp.float32) * scale[:, None]).astype(jnp.bfloat16)
        pre_gate = jnp.dot(inputs, gate_rows.T, preferred_element_type=jnp.float32)
        pre_up = jnp.dot(inputs, up_rows.T, preferred_element_type=jnp.float32)
        active, derivative = silu_parts(pre_gate)
        hidden = (active * pre_up).astype(jnp.bfloat16)
        grad_hidden = jnp.dot(grads_out, down_rows.T, preferred_element_type=jnp.float32)
        grad_gate = (grad_hidden * pre_up * derivative).astype(jnp.bfloat16)
        grad_up = (grad_hidden * active).astype(jnp.bfloat16)
        down_grad = jnp.dot(hidden.T, grads_out, preferred_element_type=jnp.float32).astype(jnp.bfloat16)
        gate_grad = jnp.dot(grad_gate.T, inputs, preferred_element_type=jnp.float32).astype(jnp.bfloat16)
        up_grad = jnp.dot(grad_up.T, inputs, preferred_element_type=jnp.float32).astype(jnp.bfloat16)

        def add_slice(index, total):
            first = (index * width_slice).astype(jnp.int32)
            piece_gate = lax.dynamic_slice_in_dim(grad_gate, first, width_slice, 1)
            piece_up = lax.dynamic_slice_in_dim(grad_up, first, width_slice, 1)
            block_gate = lax.dynamic_slice_in_dim(gate_rows, first, width_slice, 0)
            block_up = lax.dynamic_slice_in_dim(up_rows, first, width_slice, 0)
            part = jnp.dot(piece_gate, block_gate, preferred_element_type=jnp.float32) + jnp.dot(piece_up, block_up, preferred_element_type=jnp.float32)
            rounded = lax.optimization_barrier(part.astype(jnp.bfloat16))
            return total + rounded.astype(jnp.float32)

        row_total = lax.fori_loop(0, slices, add_slice, jnp.zeros((limit, D), jnp.float32))
        return gate_grad, up_grad, down_grad, row_total.astype(jnp.bfloat16)

    grad_gate_all, grad_up_all, grad_down_all, row_grads = lax.map(one_expert, (table, filled, w_gate, w_up, w_down))
    token_rows = (table // choices_per).reshape(-1)
    masked = jnp.where(filled.reshape(-1)[:, None], row_grads.reshape(-1, D).astype(jnp.float32), jnp.zeros((), jnp.float32))
    grad_tokens = jnp.zeros((TOKENS, D), jnp.float32).at[token_rows].add(masked).astype(jnp.bfloat16)
    return grad_tokens, grad_gate_all, grad_up_all, grad_down_all
```

```python
import jax
import jax.numpy as jnp
from jax import lax
from jax.sharding import PartitionSpec as P

CAP = 6


def silu_parts(pre_gate):
    gate_prob = jax.nn.sigmoid(pre_gate)
    return (pre_gate * gate_prob, gate_prob * (1.0 + pre_gate * (1.0 - gate_prob)))


def expert_rows(inputs, grads_out, w_gate, w_up, w_down):
    pre_gate = jnp.einsum("rjcd,jfd->rjcf", inputs, w_gate, preferred_element_type=jnp.float32)
    pre_up = jnp.einsum("rjcd,jfd->rjcf", inputs, w_up, preferred_element_type=jnp.float32)
    active, derivative = silu_parts(pre_gate)
    hidden = (active * pre_up).astype(jnp.bfloat16)
    grad_hidden = jnp.einsum(
        "rjcd,jfd->rjcf", grads_out, w_down, preferred_element_type=jnp.float32
    )
    grad_gate = (grad_hidden * pre_up * derivative).astype(jnp.bfloat16)
    grad_up = (grad_hidden * active).astype(jnp.bfloat16)
    return (hidden, grad_gate, grad_up)


def weight_terms(inputs, grads_out, hidden, grad_gate, grad_up):
    term_gate = jnp.einsum("rjcf,rjcd->jfd", grad_gate, inputs, preferred_element_type=jnp.float32)
    term_up = jnp.einsum("rjcf,rjcd->jfd", grad_up, inputs, preferred_element_type=jnp.float32)
    term_down = jnp.einsum("rjcf,rjcd->jfd", hidden, grads_out, preferred_element_type=jnp.float32)
    return (term_gate, term_up, term_down)


def input_terms(grad_gate, grad_up, w_gate, w_up):
    from_gate = jnp.einsum("rjcf,jfd->rjcd", grad_gate, w_gate, preferred_element_type=jnp.float32)
    from_up = jnp.einsum("rjcf,jfd->rjcd", grad_up, w_up, preferred_element_type=jnp.float32)
    return from_gate + from_up


def send_sum(blocks, axis):
    count = lax.axis_size(axis)
    me = lax.axis_index(axis)
    total = lax.dynamic_index_in_dim(blocks, me, 0, keepdims=False).astype(jnp.float32)
    for step in range(1, count):
        outgoing = lax.dynamic_index_in_dim(blocks, (me + step) % count, 0, keepdims=False)
        perm = [(i, (i + step) % count) for i in range(count)]
        total = total + lax.ppermute(outgoing, axis, perm).astype(jnp.float32)
    return total.astype(jnp.bfloat16)


def local(tokens, cotangent, routes, gate_weights, lengths, rewards, w_gate, w_up, w_down):
    samples = lax.axis_size("sample")
    own_reward = rewards.astype(jnp.float32) * 0.0625
    reward_total = own_reward
    for step in range(1, samples):
        perm = [(i, (i + step) % samples) for i in range(samples)]
        reward_total = reward_total + lax.ppermute(own_reward, "sample", perm)
    advantage = own_reward - (reward_total - own_reward) / (samples - 1)
    token_count = tokens.shape[0]
    model_width = tokens.shape[1]
    choices_per = routes.shape[1]
    local_experts = w_gate.shape[0]
    expert_groups = lax.axis_size("expert")
    all_experts = local_experts * expert_groups
    positions = jnp.arange(token_count, dtype=jnp.int32)
    weight_row = jnp.where(positions < lengths[0, 0], -advantage[0, 0], jnp.zeros((), jnp.float32))
    pair_scale = (gate_weights * weight_row[:, None]).reshape(-1)
    pair_expert = routes.reshape(-1)
    member = (pair_expert[:, None] == jnp.arange(all_experts, dtype=jnp.int32)[None, :]).astype(
        jnp.int32
    )
    earlier = jnp.sum((jnp.cumsum(member, axis=0) - member) * member, axis=1)
    target = pair_expert * CAP + earlier
    slot_ids = jnp.arange(all_experts * CAP, dtype=jnp.int32)
    placed = target[:, None] == slot_ids[None, :]
    chosen = jnp.sum(
        placed.reshape(token_count, choices_per, -1).astype(jnp.float32), axis=1
    ).astype(jnp.bfloat16)
    slot_scale = jnp.sum(jnp.where(placed, pair_scale[:, None], jnp.zeros((), jnp.float32)), axis=0)
    sent_inputs = jnp.dot(chosen.T, tokens, preferred_element_type=jnp.float32).astype(jnp.bfloat16)
    sent_cotangent = jnp.dot(chosen.T, cotangent, preferred_element_type=jnp.float32)
    sent_grads = (sent_cotangent * slot_scale[:, None]).astype(jnp.bfloat16)
    layout = (expert_groups, local_experts, CAP, model_width)
    arrived_inputs, arrived_grads = (
        lax.all_to_all(
            sent_inputs.reshape(layout), "expert", split_axis=0, concat_axis=0, tiled=True
        ),
        lax.all_to_all(
            sent_grads.reshape(layout), "expert", split_axis=0, concat_axis=0, tiled=True
        ),
    )
    group_inputs, group_grads = (
        lax.all_gather(arrived_inputs, ("dp", "sample"), axis=0, tiled=True),
        lax.all_gather(arrived_grads, ("dp", "sample"), axis=0, tiled=True),
    )
    hidden, grad_gate, grad_up = expert_rows(group_inputs, group_grads, w_gate, w_up, w_down)
    term_gate, term_up, term_down = weight_terms(
        group_inputs, group_grads, hidden, grad_gate, grad_up
    )
    parts = input_terms(grad_gate, grad_up, w_gate, w_up).astype(jnp.bfloat16)
    dp_size = lax.axis_size("dp")
    parts = parts.reshape(dp_size, samples, all_experts * CAP, model_width)
    row_sums = send_sum(send_sum(parts, "dp"), "sample").reshape(layout)
    returned = lax.all_to_all(row_sums, "expert", split_axis=0, concat_axis=0, tiled=True)
    flat_back = returned.reshape(all_experts * CAP, model_width)
    grad_tokens = jnp.dot(chosen, flat_back, preferred_element_type=jnp.float32).astype(
        jnp.bfloat16
    )
    return (
        grad_tokens,
        term_gate.astype(jnp.bfloat16),
        term_up.astype(jnp.bfloat16),
        term_down.astype(jnp.bfloat16),
    )


def solution(mesh):
    in_specs = (
        P(("dp", "expert", "sample"), None),
        P(("dp", "expert", "sample"), None),
        P(("dp", "expert", "sample"), None),
        P(("dp", "expert", "sample"), None),
        P(("dp", "expert"), "sample"),
        P(("dp", "expert"), "sample"),
        P("expert", ("dp", "sample"), None),
        P("expert", ("dp", "sample"), None),
        P("expert", ("dp", "sample"), None),
    )
    out_specs = (
        P(("dp", "expert", "sample"), None),
        P("expert", ("dp", "sample"), None),
        P("expert", ("dp", "sample"), None),
        P("expert", ("dp", "sample"), None),
    )
    return jax.shard_map(local, mesh=mesh, in_specs=in_specs, out_specs=out_specs, check_vma=False)
```
